8 devices in a mesh: dp: 2 (over z, y), sp: 4 (over x, core).
Axes of the slice: x: 2, y: 2, z: 1, core: 2. Of those that a mesh axis runs over, the one named last changes fastest.
Arguments:
- hidden: bfloat16 [32, 2048, 1024], P('dp', 'sp'), parts along dimension 0
- positions: int32 [32, 2048], P('dp', 'sp'), parts along dimension 0
- norm_attn: float32 [4, 1024], replicated
- norm_mlp: float32 [4, 1024], replicated
- w_query: bfloat16 [4, 1024, 16, 64], replicated
- w_key: bfloat16 [4, 1024, 16, 64], replicated
- w_value: bfloat16 [4, 1024, 16, 64], replicated
- w_out: bfloat16 [4, 16, 64, 1024], replicated
- w_gate: bfloat16 [4, 1024, 4096], replicated
- w_up: bfloat16 [4, 1024, 4096], replicated
- w_down: bfloat16 [4, 4096, 1024], replicated
Outputs:
- output: bfloat16 [32, 2048, 1024], P('dp', 'sp'), parts along dimension 0
There are 2 independent parts. The reference program is written for one: setup_inputs(seed, part) draws one part's arguments, and reference() takes and returns one part's arrays. A program takes and returns all parts, laid end to end along the dimension named above; an argument that names none is the same for every part.
All inputs are finite; a program needn't handle non-finite values.
Results may differ from the reference program's by a relative error of at most 0.02.
Values are sent between devices in bfloat16 or wider.
A program may use at most 1 GiB of HBM per device.

```python
import math
import jax
import jax.numpy as jnp
from jax import lax

BATCH = 16
SEQ_LEN = 2048
MODEL_DIM = 1024
HEADS = 16
KV_HEADS = 16
HEAD_DIM = 64
FF_DIM = 4096
WINDOW = 512
LAYERS = 4
QUERY_BLOCK = 256
ROW_BLOCK = 1024

GROUP = HEADS // KV_HEADS
EPS = 1e-5
ROPE_THETA = 10000.0


def draw_weight(key_w, shape, fan_in):
    return (jax.random.normal(key_w, shape, jnp.float32) * fan_in ** -0.5).astype(jnp.bfloat16)


def setup_inputs(seed: int = 0, part: int = 0) -> dict:
    base_keys = jax.random.split(jax.random.key(seed), 16)
    part_keys = [jax.random.fold_in(base_keys[i], part) for i in range(6)]
    coefficients = jax.random.normal(part_keys[0], (BATCH, 8, MODEL_DIM), jnp.float32)
    frequency = jax.random.uniform(part_keys[1], (BATCH, 8), jnp.float32, 0.5, 3.0) / WINDOW
    phase = jax.random.uniform(part_keys[2], (BATCH, 8), jnp.float32, 0.0, 2.0 * math.pi)
    steps = jnp.arange(SEQ_LEN, dtype=jnp.float32)
    waves = jnp.cos(2.0 * math.pi * frequency[:, None, :] * steps[None, :, None] + phase[:, None, :])
    smooth = jnp.einsum('bsm,bmd->bsd', waves, coefficients) * 0.5
    noise = jax.random.normal(part_keys[3], (BATCH, SEQ_LEN, MODEL_DIM), jnp.float32)
    hidden = (smooth + 0.5 * noise).astype(jnp.bfloat16)
    start_pos = jax.random.randint(part_keys[4], (BATCH, 1), 0, 1024)
    increments = jax.random.randint(part_keys[5], (BATCH, SEQ_LEN), 1, 3)
    positions = (start_pos + jnp.cumsum(increments, axis=1) - 1).astype(jnp.int32)
    attn_width = HEADS * HEAD_DIM
    return {
        'hidden': hidden,
        'positions': positions,
        'norm_attn': 1.0 + 0.4 * jax.random.normal(base_keys[6], (LAYERS, MODEL_DIM), jnp.float32),
        'norm_mlp': 1.0 + 0.4 * jax.random.normal(base_keys[7], (LAYERS, MODEL_DIM), jnp.float32),
        'w_query': draw_weight(base_keys[8], (LAYERS, MODEL_DIM, HEADS, HEAD_DIM), MODEL_DIM),
        'w_key': draw_weight(base_keys[9], (LAYERS, MODEL_DIM, KV_HEADS, HEAD_DIM), MODEL_DIM),
        'w_value': draw_weight(base_keys[10], (LAYERS, MODEL_DIM, KV_HEADS, HEAD_DIM), MODEL_DIM),
        'w_out': draw_weight(base_keys[11], (LAYERS, HEADS, HEAD_DIM, MODEL_DIM), attn_width),
        'w_gate': draw_weight(base_keys[12], (LAYERS, MODEL_DIM, FF_DIM), MODEL_DIM),
        'w_up': draw_weight(base_keys[13], (LAYERS, MODEL_DIM, FF_DIM), MODEL_DIM),
        'w_down': draw_weight(base_keys[14], (LAYERS, FF_DIM, MODEL_DIM), FF_DIM),
    }


def rms_norm(hidden, gain):
    x_f32 = hidden.astype(jnp.float32)
    inv_rms = lax.rsqrt(jnp.mean(x_f32 * x_f32, axis=-1, keepdims=True) + EPS)
    return (x_f32 * inv_rms * gain).astype(jnp.bfloat16)


def rotate(vectors, cos_a, sin_a):
    half = vectors.shape[-1] // 2
    first = vectors[..., :half]
    second = vectors[..., half:]
    return jnp.concatenate([first * cos_a - second * sin_a, second * cos_a + first * sin_a], axis=-1)


def sequence_attention(operands):
    query, key_ext, value_ext = operands
    span = QUERY_BLOCK + WINDOW - 1
    rows = jnp.arange(QUERY_BLOCK)[:, None]
    cols = jnp.arange(span)[None, :]
    band = (cols >= rows) & (cols <= rows + WINDOW - 1)
    scale = 1.0 / math.sqrt(HEAD_DIM)

    def one_block(block_idx):
        start = block_idx * QUERY_BLOCK
        query_blk = lax.dynamic_slice_in_dim(query, start, QUERY_BLOCK, axis=0).astype(jnp.float32)
        key_blk = lax.dynamic_slice_in_dim(key_ext, start, span, axis=0).astype(jnp.float32)
        value_blk = lax.dynamic_slice_in_dim(value_ext, start, span, axis=0).astype(jnp.float32)
        scores = jnp.einsum('qhgd,khd->hgqk', query_blk, key_blk) * scale
        valid = band & (start + cols >= WINDOW - 1)
        scores = jnp.where(valid, scores, -1e30)
        probabilities = jax.nn.softmax(scores, axis=-1).astype(jnp.bfloat16).astype(jnp.float32)
        return jnp.einsum('hgqk,khd->qhgd', probabilities, value_blk).astype(jnp.bfloat16)

    blocks = lax.map(one_block, jnp.arange(SEQ_LEN // QUERY_BLOCK))
    return blocks.reshape(SEQ_LEN, HEADS * HEAD_DIM)


def decoder_layer(hidden, params, cos_rows, sin_rows):
    norm_attn, norm_mlp, w_query, w_key, w_value, w_out, w_gate, w_up, w_down = params
    n_groups = BATCH * SEQ_LEN // ROW_BLOCK
    row_groups = hidden.reshape(n_groups, ROW_BLOCK, MODEL_DIM)
    wq_flat = w_query.reshape(MODEL_DIM, HEADS * HEAD_DIM)
    wk_flat = w_key.reshape(MODEL_DIM, KV_HEADS * HEAD_DIM)
    wv_flat = w_value.reshape(MODEL_DIM, KV_HEADS * HEAD_DIM)
    wo_flat = w_out.reshape(HEADS * HEAD_DIM, MODEL_DIM)

    def project(operands):
        rows_x, cos_g, sin_g = operands
        normed = rms_norm(rows_x, norm_attn)
        query = jnp.dot(normed, wq_flat, preferred_element_type=jnp.float32).reshape(ROW_BLOCK, HEADS, HEAD_DIM)
        key_r = jnp.dot(normed, wk_flat, preferred_element_type=jnp.float32).reshape(ROW_BLOCK, KV_HEADS, HEAD_DIM)
        value_r = jnp.dot(normed, wv_flat, preferred_element_type=jnp.float32).astype(jnp.bfloat16)
        return (rotate(query, cos_g, sin_g).astype(jnp.bfloat16),
                rotate(key_r, cos_g, sin_g).astype(jnp.bfloat16), value_r)

    query, key_r, value_r = lax.map(project, (row_groups, cos_rows, sin_rows))
    zero_rows = jnp.zeros((BATCH, WINDOW - 1, KV_HEADS, HEAD_DIM), jnp.bfloat16)
    key_ext = jnp.concatenate([zero_rows, key_r.reshape(BATCH, SEQ_LEN, KV_HEADS, HEAD_DIM)], axis=1)
    value_ext = jnp.concatenate([zero_rows, value_r.reshape(BATCH, SEQ_LEN, KV_HEADS, HEAD_DIM)], axis=1)
    query = query.reshape(BATCH, SEQ_LEN, KV_HEADS, GROUP, HEAD_DIM)
    attended = lax.map(sequence_attention, (query, key_ext, value_ext))
    attended = attended.reshape(n_groups, ROW_BLOCK, HEADS * HEAD_DIM)

    def finish(operands):
        rows_x, rows_att = operands
        mixed = (rows_x.astype(jnp.float32) + jnp.dot(rows_att, wo_flat, preferred_element_type=jnp.float32)).astype(jnp.bfloat16)
        normed = rms_norm(mixed, norm_mlp)
        gate = jnp.dot(normed, w_gate, preferred_element_type=jnp.float32).astype(jnp.bfloat16).astype(jnp.float32)
        up_proj = jnp.dot(normed, w_up, preferred_element_type=jnp.float32).astype(jnp.bfloat16).astype(jnp.float32)
        hidden_act = (jax.nn.silu(gate) * up_proj).astype(jnp.bfloat16)
        return (mixed.astype(jnp.float32) + jnp.dot(hidden_act, w_down, preferred_element_type=jnp.float32)).astype(jnp.bfloat16)

    return lax.map(finish, (row_groups, attended)).reshape(BATCH, SEQ_LEN, MODEL_DIM)


def reference(hidden, positions, norm_attn, norm_mlp, w_query, w_key, w_value, w_out, w_gate, w_up, w_down):
    half = HEAD_DIM // 2
    inv_freq = ROPE_THETA ** (-2.0 * jnp.arange(half, dtype=jnp.float32) / HEAD_DIM)
    angle = positions.astype(jnp.float32)[..., None, None] * inv_freq
    n_groups = BATCH * SEQ_LEN // ROW_BLOCK
    cos_rows = jnp.cos(angle).reshape(n_groups, ROW_BLOCK, 1, half)
    sin_rows = jnp.sin(angle).reshape(n_groups, ROW_BLOCK, 1, half)

    def body(carry, params):
        return decoder_layer(carry, params, cos_rows, sin_rows), None

    result, _ = lax.scan(body, hidden, (norm_attn, norm_mlp, w_query, w_key, w_value, w_out, w_gate, w_up, w_down))
    return result
```

```python
import functools
import math
import jax
import jax.numpy as jnp
from jax import lax
from jax.experimental import pallas as pl
from jax.experimental.pallas import tpu as pltpu
from jax.sharding import PartitionSpec as P

EPS = 1e-5
ROPE_THETA = 10000.0
WINDOW = 512
HEADS = 16
HEAD_DIM = 64
HALF = HEAD_DIM // 2
QB = 256
TM = 512
FC = 1024
F32 = jnp.float32
BF16 = jnp.bfloat16
NT = (((1,), (1,)), ((), ()))
NEG = -1e30
EXP2_SCALE = math.log2(math.e) / math.sqrt(HEAD_DIM)
VMEM_LIMIT = 64 * 1024 * 1024 - 65536


def rms_norm(x_f32, gain):
    inv_rms = lax.rsqrt(jnp.mean(x_f32 * x_f32, axis=-1, keepdims=True) + EPS)
    return (x_f32 * inv_rms * gain).astype(BF16)


def resident(shape, index):
    return pl.BlockSpec(shape, index, pipeline_mode=pl.Buffered(1))


def qkv_kernel(x_ref, g_ref, cos_t_ref, sin_t_ref, cos_ref, sin_ref, wq_ref, wk_ref, wv_ref, q_ref, k_ref, v_ref):
    h = rms_norm(x_ref[...].astype(F32), g_ref[...])
    cos_t, sin_t = cos_t_ref[...], sin_t_ref[...]
    for g in range(HEADS // 4):
        r0 = 4 * HEAD_DIM * g
        rows = slice(r0, r0 + 4 * HEAD_DIM)
        q = lax.dot_general(wq_ref[rows, :], h, NT, preferred_element_type=F32)
        for j in range(4):
            a, b = q[HEAD_DIM * j:HEAD_DIM * j + HALF], q[HEAD_DIM * j + HALF:HEAD_DIM * (j + 1)]
            q_ref[r0 + HEAD_DIM * j:r0 + HEAD_DIM * j + HALF, :] = (a * cos_t - b * sin_t).astype(BF16)
            q_ref[r0 + HEAD_DIM * j + HALF:r0 + HEAD_DIM * (j + 1), :] = (b * cos_t + a * sin_t).astype(BF16)
        wk = jnp.concatenate(
            [wk_ref[r0 + HEAD_DIM * j + HALF * p:r0 + HEAD_DIM * j + HALF * (p + 1), :] for p in range(2) for j in range(4)], axis=0)
        k = lax.dot_general(h, wk, NT, preferred_element_type=F32)
        a, b = k[:, :128], k[:, 128:]
        cos, sin = cos_ref[...], sin_ref[...]
        k_ref[:, r0:r0 + 128] = (a * cos - b * sin).astype(BF16)
        k_ref[:, r0 + 128:r0 + 256] = (b * cos + a * sin).astype(BF16)
        v_ref[rows, :] = lax.dot_general(wv_ref[rows, :], h, NT, preferred_element_type=F32).astype(BF16)


def qkv_call(layer, x, gain, tables, wq, wk, wv):
    tokens, dim = x.shape
    weight = resident((None, dim, dim), lambda i: (layer, 0, 0))
    return pl.pallas_call(
        qkv_kernel,
        out_shape=(jax.ShapeDtypeStruct((dim, tokens), BF16), jax.ShapeDtypeStruct((tokens, dim), BF16),
                   jax.ShapeDtypeStruct((dim, tokens), BF16)),
        grid=(tokens // TM,),
        in_specs=[pl.BlockSpec((TM, dim), lambda i: (i, 0)),
                  pl.BlockSpec((None, 1, dim), lambda i: (layer, 0, 0)),
                  pl.BlockSpec((HALF, TM), lambda i: (0, i)), pl.BlockSpec((HALF, TM), lambda i: (0, i)),
                  pl.BlockSpec((TM, 128), lambda i: (i, 0)), pl.BlockSpec((TM, 128), lambda i: (i, 0)),
                  weight, weight, weight],
        out_specs=(pl.BlockSpec((dim, TM), lambda i: (0, i)), pl.BlockSpec((TM, dim), lambda i: (i, 0)),
                   pl.BlockSpec((dim, TM), lambda i: (0, i))),
        compiler_params=pltpu.CompilerParams(vmem_limit_bytes=VMEM_LIMIT),
        name="qkv",
    )(x, gain, *tables, wq, wk, wv)


def attend_head(head, blk, n_blocks, tri, q_ref, k_ref, v_ref, ot_ref):
    g, j = divmod(head, 4)
    r0 = head * HEAD_DIM
    parts = []
    for piece in (q_ref[r0:r0 + HALF, :], q_ref[r0 + HALF:r0 + HEAD_DIM, :]):
        parts += [piece if n == j else jnp.zeros((HALF, QB), BF16) for n in range(4)]
    rhs = jnp.concatenate(parts, axis=0)

    def scores(back):
        start = pl.multiple_of((blk - back) * QB, QB)
        return jnp.dot(k_ref[pl.ds(start, QB), 256 * g:256 * g + 256], rhs, preferred_element_type=F32)

    def values(back):
        start = pl.multiple_of((blk - back) * QB, QB)
        return v_ref[r0:r0 + HEAD_DIM, pl.ds(start, QB)]

    own = scores(0)
    far = scores(2) if n_blocks == 3 else None
    mid = scores(1) if n_blocks >= 2 else None
    p_own = [[None, None], [None, None]]
    p_far = [[None, None], [None, None]]
    p_mid, sums = [], []
    for c in range(2):
        cols = slice(128 * c, 128 * c + 128)
        tiles = []
        for a in range(2):
            rows = slice(128 * a, 128 * a + 128)
            if a == c:
                tiles.append(jnp.where(tri, own[rows, cols], far[rows, cols] if far is not None else NEG))
            elif a < c:
                tiles.append(own[rows, cols])
            else:
                tiles.append(far[rows, cols] if far is not None else None)
        if mid is not None:
            tiles.append(mid[:, cols])
        top = functools.reduce(jnp.maximum, [jnp.max(t, axis=0, keepdims=True) for t in tiles if t is not None])
        total = 0.0
        for a, t in enumerate(tiles):
            if t is None:
                continue
            p = jnp.exp2((t - top) * EXP2_SCALE)
            total = total + jnp.sum(p, axis=0, keepdims=True)
            if a == 2:
                p_mid.append(p.astype(BF16))
            elif a == c:
                p_own[a][c] = jnp.where(tri, p, 0.0).astype(BF16)
                p_far[a][c] = jnp.where(tri, 0.0, p).astype(BF16)
            elif a < c:
                p_own[a][c] = p.astype(BF16)
            else:
                p_far[a][c] = p.astype(BF16)
        sums.append(total)
    zero = jnp.zeros((128, 128), BF16)

    def tile(p):
        return jnp.concatenate([jnp.concatenate([zero if t is None else t for t in row], axis=1) for row in p], axis=0)

    out = jnp.dot(values(0), tile(p_own), preferred_element_type=F32)
    if mid is not None:
        out = out + jnp.dot(values(1), jnp.concatenate(p_mid, axis=1), preferred_element_type=F32)
    if far is not None:
        out = out + jnp.dot(values(2), tile(p_far), preferred_element_type=F32)
    ot_ref[r0:r0 + HEAD_DIM, :] = (out * (1.0 / jnp.concatenate(sums, axis=1))).astype(BF16)


def attention_kernel(x_ref, q_ref, k_ref, v_ref, wo_ref, o_ref, ot_ref):
    blk = pl.program_id(1)
    tri = lax.broadcasted_iota(jnp.int32, (128, 128), 0) <= lax.broadcasted_iota(jnp.int32, (128, 128), 1)

    def run(n_blocks):
        for head in range(HEADS):
            attend_head(head, blk, n_blocks, tri, q_ref, k_ref, v_ref, ot_ref)

    pl.when(blk == 0)(lambda: run(1))
    pl.when(blk == 1)(lambda: run(2))
    pl.when(blk >= 2)(lambda: run(3))
    y = jnp.dot(jnp.transpose(ot_ref[...]), wo_ref[...], preferred_element_type=F32)
    o_ref[...] = (x_ref[...].astype(F32) + y).astype(BF16)


def attention_call(layer, seq, x, q, k, v, wo):
    tokens, dim = x.shape
    n = seq // QB
    return pl.pallas_call(
        attention_kernel,
        out_shape=jax.ShapeDtypeStruct((tokens, dim), BF16),
        grid=(tokens // seq, n),
        in_specs=[pl.BlockSpec((QB, dim), lambda b, i: (b * n + i, 0)),
                  pl.BlockSpec((dim, QB), lambda b, i: (0, b * n + i)),
                  pl.BlockSpec((seq, dim), lambda b, i: (b, 0)),
                  pl.BlockSpec((dim, seq), lambda b, i: (0, b)),
                  resident((None, dim, dim), lambda b, i: (layer, 0, 0))],
        out_specs=pl.BlockSpec((QB, dim), lambda b, i: (b * n + i, 0)),
        scratch_shapes=[pltpu.VMEM((dim, QB), BF16)],
        compiler_params=pltpu.CompilerParams(vmem_limit_bytes=VMEM_LIMIT),
        name="attention",
    )(x, q, k, v, wo)


def mlp_kernel(x_ref, g_ref, wg_ref, wu_ref, wd_ref, o_ref, act_ref):
    h = rms_norm(x_ref[...].astype(F32), g_ref[...])
    for c in range(wg_ref.shape[1] // FC):
        cols = slice(c * FC, (c + 1) * FC)
        a = jnp.dot(h, wg_ref[:, cols], preferred_element_type=F32).astype(BF16).astype(F32)
        b = jnp.dot(h, wu_ref[:, cols], preferred_element_type=F32).astype(BF16).astype(F32)
        act_ref[:, cols] = (a * (1.0 / (1.0 + jnp.exp(-a))) * b).astype(BF16)
    y = jnp.dot(act_ref[...], wd_ref[...], preferred_element_type=F32)
    o_ref[...] = (x_ref[...].astype(F32) + y).astype(BF16)


def mlp_call(layer, x, gain, wg, wu, wd):
    tokens, dim = x.shape
    ff = wg.shape[2]
    return pl.pallas_call(
        mlp_kernel,
        out_shape=jax.ShapeDtypeStruct((tokens, dim), BF16),
        grid=(tokens // TM,),
        in_specs=[pl.BlockSpec((TM, dim), lambda i: (i, 0)),
                  pl.BlockSpec((None, 1, dim), lambda i: (layer, 0, 0)),
                  resident((None, dim, ff), lambda i: (layer, 0, 0)),
                  resident((None, dim, ff), lambda i: (layer, 0, 0)),
                  resident((None, ff, dim), lambda i: (layer, 0, 0))],
        out_specs=pl.BlockSpec((TM, dim), lambda i: (i, 0)),
        scratch_shapes=[pltpu.VMEM((TM, ff), BF16)],
        compiler_params=pltpu.CompilerParams(vmem_limit_bytes=VMEM_LIMIT),
        name="mlp",
    )(x, gain, wg, wu, wd)


def rope_tables(positions):
    inv_freq = ROPE_THETA ** (-2.0 * jnp.arange(HALF, dtype=F32) / HEAD_DIM)
    angle = positions.astype(F32)[:, None] * inv_freq
    cos, sin = jnp.cos(angle), jnp.sin(angle)
    return cos.T, sin.T, jnp.tile(cos, (1, 4)), jnp.tile(sin, (1, 4))


def solution(mesh):
    def local_stack(hidden, positions, norm_attn, norm_mlp, w_query, w_key, w_value, w_out, w_gate, w_up, w_down):
        layers, dim = norm_attn.shape
        x = lax.all_to_all(hidden, 'sp', split_axis=0, concat_axis=1, tiled=True)
        pos = lax.all_to_all(positions, 'sp', split_axis=0, concat_axis=1, tiled=True)
        n_seq, seq = pos.shape
        x = x.reshape(n_seq * seq, dim)
        tables = rope_tables(pos.reshape(-1))
        out_in = [jnp.transpose(w, (0, 2, 3, 1)).reshape(layers, dim, dim) for w in (w_query, w_key, w_value)]
        wo = w_out.reshape(layers, dim, dim)
        g1, g2 = norm_attn.reshape(layers, 1, dim), norm_mlp.reshape(layers, 1, dim)
        for layer in range(layers):
            q, k, v = qkv_call(layer, x, g1, tables, *out_in)
            x = attention_call(layer, seq, x, q, k, v, wo)
            x = mlp_call(layer, x, g2, w_gate, w_up, w_down)
        return lax.all_to_all(x.reshape(n_seq, seq, dim), 'sp', split_axis=1, concat_axis=0, tiled=True)

    row_spec = P('dp', 'sp', None)
    return jax.shard_map(local_stack, mesh=mesh,
                         in_specs=(row_spec, P('dp', 'sp'), P(), P(), P(), P(), P(), P(), P(), P(), P()),
                         out_specs=row_spec, check_vma=False)
```
